32 devices in a mesh: dp: 8 (over z, y), tensor: 4 (over x, core).
Axes of the slice: x: 2, y: 2, z: 4, core: 2. Of those that a mesh axis runs over, the one named last changes fastest.
Arguments:
- tokens: bfloat16 [16384, 768], P(('dp', 'tensor')), may hold values from -6 to 6
- lengths: int32 [8], P('dp'), may hold values from 512 to 2048, as said below
- qkv_weight: bfloat16 [3, 768, 768], P(None, 'dp', 'tensor'), may hold values from -0.21875 to 0.21875
- qv_bias: float32 [2, 768], replicated, may hold values from -0.75 to 0.75
- out_weight: bfloat16 [768, 768], P('tensor', 'dp'), may hold values from -6 to 6
- out_bias: float32 [768], replicated, may hold values from -4 to 4
- first_gain: float32 [768], replicated, may hold values from 0.5 to 1.5
- first_shift: float32 [768], replicated, may hold values from -4 to 4
- up_weight: bfloat16 [768, 3072], P('dp', 'tensor'), may hold values from -0.21875 to 0.21875
- up_bias: float32 [3072], replicated, may hold values from -6 to 6
- down_weight: bfloat16 [3072, 768], P('tensor', 'dp'), may hold values from -0.109375 to 0.109375
- down_bias: float32 [768], replicated, may hold values from -4 to 4
- second_gain: float32 [768], replicated, may hold values from 0.5 to 1.5
- second_shift: float32 [768], replicated, may hold values from -4 to 4
- cotangent: bfloat16 [16384, 768], P(('dp', 'tensor')), may hold values from -6 to 6
Outputs:
- layer_out: bfloat16 [16384, 768], P(('dp', 'tensor'))
- grad_tokens: float32 [16384, 768], P(('dp', 'tensor'))
- grad_qkv_weight: float32 [3, 768, 768], P(None, 'dp', 'tensor')
- grad_qv_bias: float32 [2, 768], P(None, ('dp', 'tensor'))
- grad_out_weight: float32 [768, 768], P('tensor', 'dp')
- grad_out_bias: float32 [768], P(('dp', 'tensor'))
- grad_first_gain: float32 [768], P(('dp', 'tensor'))
- grad_first_shift: float32 [768], P(('dp', 'tensor'))
- grad_up_weight: float32 [768, 3072], P('dp', 'tensor')
- grad_up_bias: float32 [3072], P(('dp', 'tensor'))
- grad_down_weight: float32 [3072, 768], P('tensor', 'dp')
- grad_down_bias: float32 [768], P(('dp', 'tensor'))
- grad_second_gain: float32 [768], P(('dp', 'tensor'))
- grad_second_shift: float32 [768], P(('dp', 'tensor'))
The draws below stay inside these ranges and needn't reach their ends.
Inputs may be any that keep to these rules, and one draw needn't show every extreme that they name: `lengths`: each slot's valid tokens come first; some slot is full, with 2048 valid tokens.
All inputs are finite; a program needn't handle non-finite values.
Results may differ from the reference program's by a relative error of at most 0.02.
Values may be sent and summed in bfloat16 or wider, within the bound.
A program may use at most 128 MiB of HBM per device.

```python
import math
import jax
import jax.numpy as jnp
from jax import lax

D = 768
HEADS = 12
HEAD = 64
FF = 3072
SEQ = 2048
MIN_LEN = 512
SLOTS = 8
TOKENS = 16384


def draw_lengths(key, part):
    first_key, second_key = jax.random.split(key)
    values = jax.random.randint(first_key, (SLOTS,), MIN_LEN, SEQ + 1, dtype=jnp.int32)
    place = jax.random.randint(second_key, (), 0, SLOTS, dtype=jnp.int32)
    return jnp.where(jnp.arange(SLOTS, dtype=jnp.int32) == place, jnp.int32(SEQ), values)


def steps_of(key, dims, cuts, least, largest):
    loudness, own = 1.0, jax.random.fold_in(key, 6)
    for dim, blocks in cuts:
        draws = jnp.exp(jax.random.uniform(jax.random.fold_in(own, dim), (blocks,), jnp.float32, least / len(cuts), largest / len(cuts)))
        loudness = loudness * jnp.repeat(draws, dims[dim] // blocks).reshape([-1 if axis == dim else 1 for axis in range(len(dims))])
    return loudness


def noise(rng, shape, spread, bound, cuts=(), kind=jnp.bfloat16):
    drawn = spread * jax.random.normal(rng, shape, jnp.float32)
    if cuts:
        drawn = drawn * steps_of(rng, shape, cuts, -0.22, 0.18)
    return jnp.clip(drawn, -bound, bound).astype(kind)


def setup_inputs(seed: int = 0) -> dict:
    key_list = jax.random.split(jax.random.key(seed), 16)
    tokens = noise(key_list[0], (TOKENS, D), 1.0, 6.0, ((0, 32),))
    lengths = draw_lengths(jax.random.fold_in(key_list[15], 71), 0)
    qkv_weight = noise(key_list[2], (3, D, D), D ** -0.5, 0.21875, ((1, 8), (2, 4)))
    qv_bias = noise(key_list[3], (2, D), 0.05, 0.75, (), jnp.float32)
    out_weight = noise(key_list[4], (D, D), 0.8, 6.0, ((0, 4), (1, 8)))
    out_bias = noise(key_list[5], (D,), 0.3, 4.0, (), jnp.float32)
    first_gain = jnp.clip(1.0 + 0.1 * jax.random.normal(key_list[6], (D,), jnp.float32), 0.5, 1.5)
    first_shift = noise(key_list[7], (D,), 0.3, 4.0, (), jnp.float32)
    up_weight = noise(key_list[8], (D, FF), D ** -0.5, 0.21875, ((0, 8), (1, 4)))
    up_bias = noise(key_list[9], (FF,), 0.5, 6.0, (), jnp.float32)
    down_weight = noise(key_list[10], (FF, D), FF ** -0.5, 0.109375, ((0, 4), (1, 8)))
    down_bias = noise(key_list[11], (D,), 0.3, 4.0, (), jnp.float32)
    second_gain = jnp.clip(1.0 + 0.1 * jax.random.normal(key_list[12], (D,), jnp.float32), 0.5, 1.5)
    second_shift = noise(key_list[13], (D,), 0.3, 4.0, (), jnp.float32)
    cotangent = noise(key_list[14], (TOKENS, D), 1.0, 6.0, ((0, 32),))
    return dict(tokens=tokens, lengths=lengths, qkv_weight=qkv_weight, qv_bias=qv_bias, out_weight=out_weight, out_bias=out_bias, first_gain=first_gain, first_shift=first_shift, up_weight=up_weight, up_bias=up_bias, down_weight=down_weight, down_bias=down_bias, second_gain=second_gain, second_shift=second_shift, cotangent=cotangent)


NEGATIVE = -1e+30
EPSILON = 1e-05
HIGHEST = lax.Precision.HIGHEST

@jax.custom_vjp
def low(v):
    return lax.optimization_barrier(v.astype(jnp.bfloat16)).astype(jnp.float32)

@jax.custom_vjp
def low_back(v):
    return v

def low_keep(v):
    return (low(v), None)

def low_pass(kept, grad):
    return (grad,)

def back_keep(v):
    return (v, None)

def back_low(kept, grad):
    return (low(grad),)
low.defvjp(low_keep, low_pass)
low_back.defvjp(back_keep, back_low)

def gelu_tanh(values):
    bracket = 0.7978845608028654 * (values + 0.044715 * values * values * values)
    return 0.5 * values * (1.0 + jnp.tanh(bracket))

def norm_rows(hidden, scaling, offset):
    centered = hidden - lax.optimization_barrier(jnp.mean(hidden, axis=-1, keepdims=True))
    inverse = lax.rsqrt(lax.optimization_barrier(jnp.mean(centered * centered, axis=-1, keepdims=True)) + EPSILON)
    return centered * inverse * scaling + offset

def product(left, right):
    return jnp.dot(left, right, precision=HIGHEST)

def split_heads(matrix):
    return matrix.reshape(SEQ, HEADS, HEAD).transpose(1, 0, 2)

def forward(params, rows, length):
    qkv_weight, qv_bias, out_weight, out_bias, first_gain, first_shift, up_weight, up_bias, down_weight, down_bias, second_gain, second_shift = params
    scale = 1.0 / math.sqrt(HEAD)
    key_valid = jnp.arange(SEQ, dtype=jnp.int32) < length
    queries = low(low_back(product(rows, qkv_weight[0]) + qv_bias[0]))
    key_rows = low(low_back(product(rows, qkv_weight[1])))
    value_rows = low(low_back(product(rows, qkv_weight[2]) + qv_bias[1]))

    def head_attend(operands):
        query_head, key_head, value_head = operands
        scores = product(query_head, key_head.T) * scale
        scores = low_back(jnp.where(key_valid[None, :], scores, NEGATIVE))
        top_score = lax.optimization_barrier(jnp.max(scores, axis=-1, keepdims=True))
        expo = jnp.exp(scores - top_score)
        probs = expo / lax.optimization_barrier(jnp.sum(expo, axis=-1, keepdims=True))
        return product(low(probs), value_head)
    heads_out = lax.map(jax.checkpoint(head_attend), (split_heads(queries), split_heads(key_rows), split_heads(value_rows)))
    mixed = low(low_back(heads_out.transpose(1, 0, 2).reshape(SEQ, D)))
    attn_out = low_back(product(mixed, out_weight) + out_bias)
    first = norm_rows(rows + attn_out, first_gain, first_shift)
    pre_act = low_back(product(low(first), up_weight) + up_bias)
    activated = low(gelu_tanh(pre_act))
    ffn_out = low_back(product(activated, down_weight) + down_bias)
    return norm_rows(first + ffn_out, second_gain, second_shift)

def reference(tokens, lengths, qkv_weight, qv_bias, out_weight, out_bias, first_gain, first_shift, up_weight, up_bias, down_weight, down_bias, second_gain, second_shift, cotangent):
    params = tuple((item.astype(jnp.float32) for item in (qkv_weight, qv_bias, out_weight, out_bias, first_gain, first_shift, up_weight, up_bias, down_weight, down_bias, second_gain, second_shift)))

    def one_slot(totals, inputs):
        rows, upstream, length = inputs

        def slot_forward(prm, slot_rows):
            return forward(prm, slot_rows, length)
        result, pull_back = jax.vjp(slot_forward, params, rows)
        row_mask = (jnp.arange(SEQ, dtype=jnp.int32) < length).astype(jnp.float32)[:, None]
        param_grads, row_grads = pull_back(upstream * row_mask)
        totals = jax.tree.map(jnp.add, totals, param_grads)
        return (totals, (result.astype(jnp.bfloat16), row_grads))
    zeros = jax.tree.map(jnp.zeros_like, params)
    slot_rows = tokens.astype(jnp.float32).reshape(SLOTS, SEQ, D)
    slot_upstream = cotangent.astype(jnp.float32).reshape(SLOTS, SEQ, D)
    totals, (outputs, row_grads) = lax.scan(one_slot, zeros, (slot_rows, slot_upstream, lengths))
    return (outputs.reshape(TOKENS, D), row_grads.reshape(TOKENS, D), totals[0], totals[1], totals[2], totals[3], totals[4], totals[5], totals[6], totals[7], totals[8], totals[9], totals[10], totals[11])
```

```python
import math

import jax
import jax.numpy as jnp
from jax import lax
from jax.sharding import PartitionSpec as P

HEAD = 64
NEGATIVE = -1e30
EPSILON = 1e-05
F32 = jnp.float32
BF16 = jnp.bfloat16


def gelu_tanh(values):
    bracket = 0.7978845608028654 * (values + 0.044715 * values * values * values)
    return 0.5 * values * (1.0 + jnp.tanh(bracket))


def norm_rows(hidden, scaling, offset):
    centered = hidden - jnp.mean(hidden, axis=-1, keepdims=True)
    inverse = lax.rsqrt(jnp.mean(centered * centered, axis=-1, keepdims=True) + EPSILON)
    normed = centered * inverse
    return (normed * scaling + offset, normed, inverse)


def norm_back(upstream, normed, inverse, scaling):
    scaled = upstream * scaling
    bracket = (
        scaled
        - jnp.mean(scaled, axis=-1, keepdims=True)
        - normed * jnp.mean(scaled * normed, axis=-1, keepdims=True)
    )
    return (inverse * bracket, jnp.sum(upstream * normed, axis=0), jnp.sum(upstream, axis=0))


def mm(left, right, dims):
    return lax.dot_general(left, right, (dims, ((), ())), preferred_element_type=F32)


def gather_tensor(rows):
    return lax.all_gather(rows, "tensor", axis=0, tiled=True)


def scatter_tensor(part):
    return lax.psum_scatter(part, "tensor", scatter_dimension=0, tiled=True)


def attention_forward(queries, key_rows, value_rows, length):
    total_rows, head_cols = queries.shape
    head_count = head_cols // HEAD
    scale = 1.0 / math.sqrt(HEAD)
    block = min(512, total_rows)
    blocks = total_rows // block
    key_valid = jnp.arange(total_rows, dtype=jnp.int32) < length
    key_heads = key_rows.reshape(total_rows, head_count, HEAD)
    value_heads = value_rows.reshape(total_rows, head_count, HEAD)
    query_blocks = queries.reshape(blocks, block, head_count, HEAD)

    def attend_block(query_block):
        scores = (
            jnp.einsum("qhd,khd->hqk", query_block, key_heads, preferred_element_type=F32) * scale
        )
        scores = jnp.where(key_valid[None, None, :], scores, NEGATIVE)
        top_score = jnp.max(scores, axis=-1, keepdims=True)
        expo = jnp.exp(scores - top_score)
        row_total = jnp.sum(expo, axis=-1, keepdims=True)
        probs = (expo / row_total).astype(BF16)
        context = jnp.einsum("hqk,khd->qhd", probs, value_heads, preferred_element_type=F32)
        return (context.astype(BF16), (top_score + jnp.log(row_total))[..., 0])

    context_blocks, log_totals = lax.map(attend_block, query_blocks)
    return context_blocks.reshape(total_rows, head_cols), log_totals


def attention_backward(queries, key_rows, value_rows, mixed_grad, log_totals, length):
    total_rows, head_cols = queries.shape
    head_count = head_cols // HEAD
    scale = 1.0 / math.sqrt(HEAD)
    block = min(512, total_rows)
    blocks = total_rows // block
    key_valid = jnp.arange(total_rows, dtype=jnp.int32) < length
    key_heads = key_rows.reshape(total_rows, head_count, HEAD)
    value_heads = value_rows.reshape(total_rows, head_count, HEAD)
    query_blocks = queries.reshape(blocks, block, head_count, HEAD)
    mixed_blocks = mixed_grad.reshape(blocks, block, head_count, HEAD)

    def back_block(carry, inputs):
        key_acc, value_acc = carry
        query_block, grad_block, log_total = inputs
        scores = (
            jnp.einsum("qhd,khd->hqk", query_block, key_heads, preferred_element_type=F32) * scale
        )
        scores = jnp.where(key_valid[None, None, :], scores, NEGATIVE)
        probs = jnp.exp(scores - log_total[:, :, None])
        value_acc = value_acc + jnp.einsum(
            "hqk,qhd->khd", probs.astype(BF16), grad_block, preferred_element_type=F32
        )
        prob_grad = jnp.einsum("qhd,khd->hqk", grad_block, value_heads, preferred_element_type=F32)
        centre = jnp.sum(probs * prob_grad, axis=-1, keepdims=True)
        score_grad = (probs * (prob_grad - centre)).astype(BF16)
        query_grad = (
            jnp.einsum("hqk,khd->qhd", score_grad, key_heads, preferred_element_type=F32) * scale
        )
        key_acc = (
            key_acc
            + jnp.einsum("hqk,qhd->khd", score_grad, query_block, preferred_element_type=F32)
            * scale
        )
        return ((key_acc, value_acc), query_grad.astype(BF16))

    empty = jnp.zeros((total_rows, head_count, HEAD), F32)
    (key_total, value_total), query_grads = lax.scan(
        back_block, (empty, empty), (query_blocks, mixed_blocks, log_totals)
    )
    return (
        query_grads.reshape(total_rows, head_cols),
        key_total.reshape(total_rows, head_cols).astype(BF16),
        value_total.reshape(total_rows, head_cols).astype(BF16),
    )


def per_device(
    tokens,
    lengths,
    qkv_weight,
    qv_bias,
    out_weight,
    out_bias,
    first_gain,
    first_shift,
    up_weight,
    up_bias,
    down_weight,
    down_bias,
    second_gain,
    second_shift,
    cotangent,
):
    local_rows, width = tokens.shape
    piece = lax.axis_index("tensor")
    ways = lax.axis_size("dp") * lax.axis_size("tensor")
    head_cols = qkv_weight.shape[2]
    unit_cols = up_weight.shape[1]
    depth = up_weight.shape[0]
    length = lengths[0]
    qkv_rows = jnp.concatenate([qkv_weight[0], qkv_weight[1], qkv_weight[2]], axis=1)
    qkv_full = lax.all_gather(qkv_rows, "dp", axis=0, tiled=True)
    rest_rows = jnp.concatenate([up_weight, down_weight.T, out_weight.T], axis=1)
    rest_full = lax.all_gather(rest_rows, "dp", axis=0, tiled=True)
    up_full = rest_full[:, :unit_cols]
    down_full = rest_full[:, unit_cols : 2 * unit_cols]
    out_full = rest_full[:, 2 * unit_cols :]
    seq_tokens = gather_tensor(tokens)
    row_start = piece * local_rows
    row_valid = row_start + jnp.arange(local_rows, dtype=jnp.int32) < length
    head_start = piece * head_cols
    unit_start = piece * unit_cols
    bias_cols = lax.dynamic_slice_in_dim(qv_bias, head_start, head_cols, 1)
    qkv_bias = jnp.concatenate([bias_cols[0], jnp.zeros((head_cols,), F32), bias_cols[1]])
    projected = (mm(seq_tokens, qkv_full, ((1,), (0,))) + qkv_bias).astype(BF16)
    queries = projected[:, :head_cols]
    key_rows = projected[:, head_cols : 2 * head_cols]
    value_rows = projected[:, 2 * head_cols :]
    mixed, log_totals = attention_forward(queries, key_rows, value_rows, length)
    attn_local = scatter_tensor(mm(mixed, out_full, ((1,), (1,))).astype(BF16)).astype(F32)
    first_out, first_normed, first_inverse = norm_rows(
        tokens.astype(F32) + (attn_local + out_bias), first_gain, first_shift
    )
    seq_first = gather_tensor(first_out.astype(BF16))
    up_cols = lax.dynamic_slice_in_dim(up_bias, unit_start, unit_cols, 0)
    pre_act = mm(seq_first, up_full, ((1,), (0,))) + up_cols
    activated = gelu_tanh(pre_act).astype(BF16)
    ffn_local = scatter_tensor(mm(activated, down_full, ((1,), (1,))).astype(BF16)).astype(F32)
    second_in = first_out + (ffn_local + down_bias)
    layer_out, second_normed, second_inverse = norm_rows(second_in, second_gain, second_shift)
    upstream = cotangent.astype(F32) * row_valid[:, None].astype(F32)
    grad_second, gain_two_part, shift_two_part = norm_back(
        upstream, second_normed, second_inverse, second_gain
    )
    ffn_grad = grad_second.astype(BF16)
    down_bias_part = jnp.sum(ffn_grad.astype(F32), axis=0)
    unused_value, gelu_pull = jax.vjp(gelu_tanh, pre_act)
    seq_ffn_grad = gather_tensor(ffn_grad)
    act_grad = mm(seq_ffn_grad, down_full, ((1,), (0,)))
    pre_grad = gelu_pull(act_grad)[0].astype(BF16)
    first_back = scatter_tensor(mm(pre_grad, up_full, ((1,), (1,))).astype(BF16)).astype(F32)
    up_bias_part = jnp.sum(pre_grad.astype(F32), axis=0)
    down_grad = mm(seq_ffn_grad, activated, ((0,), (0,))).astype(BF16)
    up_grad = mm(seq_first, pre_grad, ((0,), (0,))).astype(BF16)
    grad_first, gain_one_part, shift_one_part = norm_back(
        grad_second + first_back, first_normed, first_inverse, first_gain
    )
    attn_grad = grad_first.astype(BF16)
    out_bias_part = jnp.sum(attn_grad.astype(F32), axis=0)
    attn_grad, up_grad, down_grad = lax.optimization_barrier((attn_grad, up_grad, down_grad))
    grad_ud = lax.psum_scatter(
        jnp.concatenate([up_grad, down_grad], axis=1), "dp", scatter_dimension=0, tiled=True
    )
    seq_attn_grad = gather_tensor(attn_grad)
    out_grad = mm(seq_attn_grad, mixed, ((0,), (0,))).astype(BF16)
    mixed_grad = mm(seq_attn_grad, out_full, ((1,), (0,))).astype(BF16)
    query_grad, key_grad, value_grad = attention_backward(
        queries, key_rows, value_rows, mixed_grad, log_totals, length
    )
    stacked = jnp.concatenate([query_grad, key_grad, value_grad], axis=1)
    token_back = scatter_tensor(mm(stacked, qkv_full, ((1,), (1,))).astype(BF16)).astype(F32)
    qkv_grad = mm(seq_tokens, stacked, ((0,), (0,))).astype(BF16)
    grad_qo = lax.psum_scatter(
        jnp.concatenate([qkv_grad, out_grad], axis=1), "dp", scatter_dimension=0, tiled=True
    )
    grad_tokens = grad_first + token_back
    zeros_heads = jnp.zeros((width,), F32)
    query_bias = lax.dynamic_update_slice(
        zeros_heads, jnp.sum(query_grad.astype(F32), axis=0), (head_start,)
    )
    value_bias = lax.dynamic_update_slice(
        zeros_heads, jnp.sum(value_grad.astype(F32), axis=0), (head_start,)
    )
    up_bias_full = lax.dynamic_update_slice(
        jnp.zeros((up_bias.shape[0],), F32), up_bias_part, (unit_start,)
    )
    small = jnp.concatenate(
        [
            item.reshape(ways, -1)
            for item in (
                query_bias,
                value_bias,
                out_bias_part,
                gain_one_part,
                shift_one_part,
                up_bias_full,
                down_bias_part,
                gain_two_part,
                shift_two_part,
            )
        ],
        axis=1,
    )
    small = lax.psum_scatter(small, ("dp", "tensor"), scatter_dimension=0, tiled=True)[0]
    share = width // ways
    cuts = [0]
    for size in (share, share, share, share, share, up_bias.shape[0] // ways, share, share, share):
        cuts.append(cuts[-1] + size)
    bits = [small[cuts[i] : cuts[i + 1]] for i in range(9)]
    grad_ud = grad_ud.astype(F32)
    grad_qo = grad_qo.astype(F32)
    grad_qkv = jnp.stack([grad_qo[:, i * head_cols : (i + 1) * head_cols] for i in range(3)])
    return (
        layer_out.astype(BF16),
        grad_tokens,
        grad_qkv,
        jnp.stack([bits[0], bits[1]]),
        grad_qo[:, 3 * head_cols :].T,
        bits[2],
        bits[3],
        bits[4],
        grad_ud[:, :unit_cols],
        bits[5],
        grad_ud[:, unit_cols:].T,
        bits[6],
        bits[7],
        bits[8],
    )


def solution(mesh):
    both = ("dp", "tensor")
    return jax.shard_map(
        per_device,
        mesh=mesh,
        in_specs=(
            P(both, None),
            P("dp"),
            P(None, "dp", "tensor"),
            P(),
            P("tensor", "dp"),
            P(),
            P(),
            P(),
            P("dp", "tensor"),
            P(),
            P("tensor", "dp"),
            P(),
            P(),
            P(),
            P(both, None),
        ),
        out_specs=(
            P(both, None),
            P(both, None),
            P(None, "dp", "tensor"),
            P(None, both),
            P("tensor", "dp"),
            P(both),
            P(both),
            P(both),
            P("dp", "tensor"),
            P(both),
            P("tensor", "dp"),
            P(both),
            P(both),
            P(both),
        ),
        check_vma=False,
    )
```

```python
import math

import jax
import jax.numpy as jnp
from jax import lax
from jax.experimental import pallas as pl
from jax.experimental.pallas import tpu as pltpu
from jax.sharding import PartitionSpec as P

HEAD = 64
NEGATIVE = -1e30
EPSILON = 1e-05
F32 = jnp.float32
BF16 = jnp.bfloat16


def gelu_tanh(values):
    bracket = 0.7978845608028654 * (values + 0.044715 * values * values * values)
    return 0.5 * values * (1.0 + jnp.tanh(bracket))


def norm_rows(hidden, scaling, offset):
    centered = hidden - jnp.mean(hidden, axis=-1, keepdims=True)
    inverse = lax.rsqrt(jnp.mean(centered * centered, axis=-1, keepdims=True) + EPSILON)
    normed = centered * inverse
    return (normed * scaling + offset, normed, inverse)


def norm_back(upstream, normed, inverse, scaling):
    scaled = upstream * scaling
    bracket = (
        scaled
        - jnp.mean(scaled, axis=-1, keepdims=True)
        - normed * jnp.mean(scaled * normed, axis=-1, keepdims=True)
    )
    return (inverse * bracket, jnp.sum(upstream * normed, axis=0), jnp.sum(upstream, axis=0))


def mm(left, right, dims):
    return lax.dot_general(left, right, (dims, ((), ())), preferred_element_type=F32)


MESH = pl.DeviceIdType.MESH
PARTS = 4
STEPS = 4


def remote(src, dst, send, recv, where):
    return pltpu.make_async_remote_copy(
        src_ref=src, dst_ref=dst, send_sem=send, recv_sem=recv, device_id=where, device_id_type=MESH
    )


def neighbours():
    me = lax.axis_index("tensor")
    partner = me + 1 - 2 * (me % 2)
    return me, partner, (me + 2) % PARTS, (partner + 2) % PARTS


def greet(count, where):
    barrier = pltpu.get_barrier_semaphore()

    def one(k, carry):
        pl.semaphore_signal(barrier, inc=1, device_id=where(k), device_id_type=MESH)
        return carry

    lax.fori_loop(0, count, one, 0)
    pl.semaphore_wait(barrier, count)


def loop(count, body):
    def step(k, carry):
        body(k)
        return carry

    lax.fori_loop(0, count, step, 0)


class RowGather:
    semaphores = [pltpu.SemaphoreType.DMA((2, STEPS))] * 2 + [pltpu.SemaphoreType.DMA((2,))]

    def __init__(self, mine, seq, cross_sems, relay_sems, own_sems):
        self.mine, self.seq = mine, seq
        self.cross_sems, self.relay_sems, self.own_sems = cross_sems, relay_sems, own_sems
        self.me, self.partner, self.cross, self.diag = neighbours()
        self.rows = mine.shape[0] // STEPS

    def cut(self, k):
        return pl.ds(pl.multiple_of(k * self.rows, self.rows), self.rows)

    def crossing(self, k):
        return remote(
            self.mine.at[self.cut(k)],
            self.seq.at[self.me, self.cut(k)],
            self.cross_sems.at[0, k],
            self.cross_sems.at[1, k],
            {"tensor": self.cross},
        )

    def relay(self, k):
        block = self.seq.at[self.cross, self.cut(k)]
        return remote(
            block,
            block,
            self.relay_sems.at[0, k],
            self.relay_sems.at[1, k],
            {"tensor": self.partner},
        )

    def own(self):
        return remote(
            self.mine,
            self.seq.at[self.me],
            self.own_sems.at[0],
            self.own_sems.at[1],
            {"tensor": self.partner},
        )

    def start(self):
        loop(STEPS, lambda k: self.crossing(k).start())
        self.own().start()
        self.seq[self.me] = self.mine[...]

    def finish(self):
        def arrive(k):
            self.crossing(k).wait_recv()
            self.relay(k).start()

        loop(STEPS, arrive)
        self.own().wait()
        loop(STEPS, lambda k: self.crossing(k).wait_send())
        loop(STEPS, lambda k: self.relay(k).wait())


def greet_pair():
    me, partner, cross, diag = neighbours()
    greet(2, lambda k: {"tensor": partner + k * (cross - partner)})


def vmem():
    return pl.BlockSpec(memory_space=pltpu.VMEM)


def gather_kernel(mine, seq, cross_sems, relay_sems, own_sems):
    greet_pair()
    rows = RowGather(mine, seq, cross_sems, relay_sems, own_sems)
    rows.start()
    rows.finish()


def gather_tensor(rows, ident):
    count, width = rows.shape
    size = PARTS * count * width * 2
    seq = pl.pallas_call(
        gather_kernel,
        out_shape=jax.ShapeDtypeStruct((PARTS, count, width), rows.dtype),
        in_specs=[vmem()],
        out_specs=vmem(),
        scratch_shapes=RowGather.semaphores,
        cost_estimate=pl.CostEstimate(flops=0, bytes_accessed=20 * size, transcendentals=0),
        compiler_params=pltpu.CompilerParams(collective_id=ident, has_side_effects=True),
        name=f"gather_rows_{ident}",
    )(rows)
    return seq.reshape(PARTS * count, width)


def start_kernel(tokens, weight, seq, full, cross_sems, relay_sems, own_sems, weight_sems):
    place, count = lax.axis_index("dp"), lax.axis_size("dp")
    me, partner, cross, diag = neighbours()
    barrier = pltpu.get_barrier_semaphore()
    for where in (partner, cross):
        pl.semaphore_signal(barrier, inc=1, device_id={"tensor": where}, device_id_type=MESH)
    loop(
        count - 1,
        lambda k: pl.semaphore_signal(
            barrier, inc=1, device_id={"dp": (place + 1 + k) % count}, device_id_type=MESH
        ),
    )
    pl.semaphore_wait(barrier, count + 1)
    rows = RowGather(tokens, seq, cross_sems, relay_sems, own_sems)

    def piece(k):
        return remote(
            weight,
            full.at[place],
            weight_sems.at[0, k],
            weight_sems.at[1, k],
            {"dp": (place + 1 + k) % count},
        )

    loop(count - 1, lambda k: piece(k).start())
    rows.start()
    full[place] = weight[...]
    rows.finish()
    loop(count - 1, lambda k: piece(k).wait())


def start_gather(tokens, weight):
    count, width = tokens.shape
    ways = lax.axis_size("dp")
    seq, full = pl.pallas_call(
        start_kernel,
        out_shape=(
            jax.ShapeDtypeStruct((PARTS, count, width), tokens.dtype),
            jax.ShapeDtypeStruct((ways,) + weight.shape, weight.dtype),
        ),
        in_specs=[vmem()] * 2,
        out_specs=(vmem(), vmem()),
        scratch_shapes=RowGather.semaphores + [pltpu.SemaphoreType.DMA((2, ways - 1))],
        cost_estimate=pl.CostEstimate(flops=0, bytes_accessed=60 << 20, transcendentals=0),
        compiler_params=pltpu.CompilerParams(collective_id=1, has_side_effects=True),
        name="start_gather",
    )(tokens, weight)
    return seq.reshape(PARTS * count, width), full.reshape(-1, weight.shape[1])


class Scatter:
    def __init__(self, left, weight, out, pair_out, pair_in, over_out, over_in, pair_sems, over_sems):
        self.left, self.weight, self.out = left, weight, out
        self.pair_out, self.pair_in = pair_out, pair_in
        self.over_out, self.over_in = over_out, over_in
        self.pair_sems, self.over_sems = pair_sems, over_sems
        self.me, self.partner, self.cross, self.diag = neighbours()
        self.rows = left.shape[1] // STEPS

    @staticmethod
    def scratch(rows, width):
        return [
            pltpu.VMEM((2, rows, width), BF16),
            pltpu.VMEM((2, rows, width), BF16),
            pltpu.VMEM((rows, width), BF16),
            pltpu.VMEM((rows, width), BF16),
            pltpu.SemaphoreType.DMA((2, 2, STEPS)),
            pltpu.SemaphoreType.DMA((2, STEPS)),
        ]

    def cut(self, k):
        return pl.ds(pl.multiple_of(k * self.rows, self.rows), self.rows)

    def pair(self, which, k):
        return remote(
            self.pair_out.at[which, self.cut(k)],
            self.pair_in.at[which, self.cut(k)],
            self.pair_sems.at[0, which, k],
            self.pair_sems.at[1, which, k],
            {"tensor": self.partner},
        )

    def over(self, k):
        return remote(
            self.over_out.at[self.cut(k)],
            self.over_in.at[self.cut(k)],
            self.over_sems.at[0, k],
            self.over_sems.at[1, k],
            {"tensor": self.cross},
        )

    def product(self, block, k):
        return mm(self.left[block, self.cut(k)], self.weight[...], ((1,), (1,)))

    def run(self):
        def away(which, block):
            def body(k):
                self.pair_out[which, self.cut(k)] = self.product(block, k).astype(BF16)
                self.pair(which, k).start()

            return body

        def across(k):
            part = self.product(self.cross, k)
            self.pair(0, k).wait_recv()
            part = part + self.pair_in[0, self.cut(k)].astype(F32)
            self.over_out[self.cut(k)] = part.astype(BF16)
            self.over(k).start()

        def home(k):
            part = self.product(self.me, k)
            self.pair(1, k).wait_recv()
            self.out[self.cut(k)] = part + self.pair_in[1, self.cut(k)].astype(F32)

        def close(k):
            self.over(k).wait_recv()
            self.out[self.cut(k)] = self.out[self.cut(k)] + self.over_in[self.cut(k)].astype(F32)

        loop(STEPS, away(0, self.diag))
        loop(STEPS, across)
        loop(STEPS, away(1, self.partner))
        loop(STEPS, home)
        loop(STEPS, close)
        for which in range(2):
            loop(STEPS, lambda k: self.pair(which, k).wait_send())
        loop(STEPS, lambda k: self.over(k).wait_send())


def scatter_kernel(left, weight, out, *scratch):
    greet_pair()
    Scatter(left, weight, out, *scratch).run()


def scatter_tensor(left, weight, ident):
    rows, inner = left.shape[0] // PARTS, left.shape[1]
    width = weight.shape[0]
    return pl.pallas_call(
        scatter_kernel,
        out_shape=jax.ShapeDtypeStruct((rows, width), F32),
        in_specs=[vmem()] * 2,
        out_specs=vmem(),
        scratch_shapes=Scatter.scratch(rows, width),
        cost_estimate=pl.CostEstimate(
            flops=2 * PARTS * rows * inner * width, bytes_accessed=60 << 20, transcendentals=0
        ),
        compiler_params=pltpu.CompilerParams(collective_id=ident, has_side_effects=True),
        name=f"scatter_rows_{ident}",
    )(left.reshape(PARTS, rows, inner), weight)


def tail_kernel(left, weight, grads, small, out, grads_out, small_out, *scratch):
    scatter_scratch, (grads_in, small_in, grad_sems, small_sems) = scratch[:6], scratch[6:]
    place, count = lax.axis_index("dp"), lax.axis_size("dp")
    me = place * PARTS + lax.axis_index("tensor")
    ways = count * PARTS

    def rank(k):
        peer = (me + 1 + k) % ways
        return {"dp": peer // PARTS, "tensor": peer % PARTS}

    greet(ways - 1, rank)

    def grad(k):
        peer = (place + 1 + k) % count
        return remote(
            grads.at[peer], grads_in.at[k], grad_sems.at[0, k], grad_sems.at[1, k], {"dp": peer}
        )

    def bit(k):
        peer = (me + 1 + k) % ways
        return remote(
            small.at[peer], small_in.at[k], small_sems.at[0, k], small_sems.at[1, k], rank(k)
        )

    loop(count - 1, lambda k: grad(k).start())
    loop(ways - 1, lambda k: bit(k).start())
    Scatter(left, weight, out, *scatter_scratch).run()
    small_out[...] = small[me]

    def add_bit(k):
        bit(k).wait()
        small_out[...] = small_out[...] + small_in[k]

    loop(ways - 1, add_bit)
    grads_out[...] = grads[place].astype(F32)

    def add_grad(k):
        grad(k).wait()
        grads_out[...] = grads_out[...] + grads_in[k].astype(F32)

    loop(count - 1, add_grad)


def tail(left, weight, grads, small):
    rows, inner = left.shape[0] // PARTS, left.shape[1]
    width = weight.shape[0]
    count, ways = grads.shape[0], small.shape[0]
    return pl.pallas_call(
        tail_kernel,
        out_shape=(
            jax.ShapeDtypeStruct((rows, width), F32),
            jax.ShapeDtypeStruct(grads.shape[1:], F32),
            jax.ShapeDtypeStruct(small.shape[1:], F32),
        ),
        in_specs=[vmem()] * 4,
        out_specs=(vmem(),) * 3,
        scratch_shapes=Scatter.scratch(rows, width)
        + [
            pltpu.VMEM((count - 1,) + grads.shape[1:], BF16),
            pltpu.VMEM((ways - 1,) + small.shape[1:], F32),
            pltpu.SemaphoreType.DMA((2, count - 1)),
            pltpu.SemaphoreType.DMA((2, ways - 1)),
        ],
        cost_estimate=pl.CostEstimate(
            flops=2 * PARTS * rows * inner * width, bytes_accessed=90 << 20, transcendentals=0
        ),
        compiler_params=pltpu.CompilerParams(collective_id=9, has_side_effects=True),
        name="tail",
    )(left.reshape(PARTS, rows, inner), weight, grads, small)


def attention_forward(queries, key_rows, value_rows, length):
    total_rows, head_cols = queries.shape
    head_count = head_cols // HEAD
    scale = 1.0 / math.sqrt(HEAD)
    block = min(512, total_rows)
    blocks = total_rows // block
    key_valid = jnp.arange(total_rows, dtype=jnp.int32) < length
    key_heads = key_rows.reshape(total_rows, head_count, HEAD)
    value_heads = value_rows.reshape(total_rows, head_count, HEAD)
    query_blocks = queries.reshape(blocks, block, head_count, HEAD)

    def attend_block(query_block):
        scores = (
            jnp.einsum("qhd,khd->hqk", query_block, key_heads, preferred_element_type=F32) * scale
        )
        scores = jnp.where(key_valid[None, None, :], scores, NEGATIVE)
        top_score = jnp.max(scores, axis=-1, keepdims=True)
        expo = jnp.exp(scores - top_score)
        row_total = jnp.sum(expo, axis=-1, keepdims=True)
        probs = (expo / row_total).astype(BF16)
        context = jnp.einsum("hqk,khd->qhd", probs, value_heads, preferred_element_type=F32)
        return (context.astype(BF16), (top_score + jnp.log(row_total))[..., 0])

    context_blocks, log_totals = lax.map(attend_block, query_blocks)
    return context_blocks.reshape(total_rows, head_cols), log_totals


def attention_backward(queries, key_rows, value_rows, mixed_grad, log_totals, length):
    total_rows, head_cols = queries.shape
    head_count = head_cols // HEAD
    scale = 1.0 / math.sqrt(HEAD)
    block = min(512, total_rows)
    blocks = total_rows // block
    key_valid = jnp.arange(total_rows, dtype=jnp.int32) < length
    key_heads = key_rows.reshape(total_rows, head_count, HEAD)
    value_heads = value_rows.reshape(total_rows, head_count, HEAD)
    query_blocks = queries.reshape(blocks, block, head_count, HEAD)
    mixed_blocks = mixed_grad.reshape(blocks, block, head_count, HEAD)

    def back_block(carry, inputs):
        key_acc, value_acc = carry
        query_block, grad_block, log_total = inputs
        scores = (
            jnp.einsum("qhd,khd->hqk", query_block, key_heads, preferred_element_type=F32) * scale
        )
        scores = jnp.where(key_valid[None, None, :], scores, NEGATIVE)
        probs = jnp.exp(scores - log_total[:, :, None])
        value_acc = value_acc + jnp.einsum(
            "hqk,qhd->khd", probs.astype(BF16), grad_block, preferred_element_type=F32
        )
        prob_grad = jnp.einsum("qhd,khd->hqk", grad_block, value_heads, preferred_element_type=F32)
        centre = jnp.sum(probs * prob_grad, axis=-1, keepdims=True)
        score_grad = (probs * (prob_grad - centre)).astype(BF16)
        query_grad = (
            jnp.einsum("hqk,khd->qhd", score_grad, key_heads, preferred_element_type=F32) * scale
        )
        key_acc = (
            key_acc
            + jnp.einsum("hqk,qhd->khd", score_grad, query_block, preferred_element_type=F32)
            * scale
        )
        return ((key_acc, value_acc), query_grad.astype(BF16))

    empty = jnp.zeros((total_rows, head_count, HEAD), F32)
    (key_total, value_total), query_grads = lax.scan(
        back_block, (empty, empty), (query_blocks, mixed_blocks, log_totals)
    )
    return (
        query_grads.reshape(total_rows, head_cols),
        key_total.reshape(total_rows, head_cols).astype(BF16),
        value_total.reshape(total_rows, head_cols).astype(BF16),
    )


def per_device(
    tokens,
    lengths,
    qkv_weight,
    qv_bias,
    out_weight,
    out_bias,
    first_gain,
    first_shift,
    up_weight,
    up_bias,
    down_weight,
    down_bias,
    second_gain,
    second_shift,
    cotangent,
):
    local_rows, width = tokens.shape
    piece = lax.axis_index("tensor")
    ways = lax.axis_size("dp") * lax.axis_size("tensor")
    head_cols = qkv_weight.shape[2]
    unit_cols = up_weight.shape[1]
    depth = up_weight.shape[0]
    length = lengths[0]
    qkv_rows = jnp.concatenate([qkv_weight[0], qkv_weight[1], qkv_weight[2]], axis=1)
    seq_tokens, qkv_full = start_gather(tokens, qkv_rows)
    rest_rows = jnp.concatenate([up_weight, down_weight.T, out_weight.T], axis=1)
    rest_full = lax.all_gather(rest_rows, "dp", axis=0, tiled=True)
    up_full = rest_full[:, :unit_cols]
    down_full = rest_full[:, unit_cols : 2 * unit_cols]
    out_full = rest_full[:, 2 * unit_cols :]
    row_start = piece * local_rows
    row_valid = row_start + jnp.arange(local_rows, dtype=jnp.int32) < length
    head_start = piece * head_cols
    unit_start = piece * unit_cols
    bias_cols = lax.dynamic_slice_in_dim(qv_bias, head_start, head_cols, 1)
    qkv_bias = jnp.concatenate([bias_cols[0], jnp.zeros((head_cols,), F32), bias_cols[1]])
    projected = (mm(seq_tokens, qkv_full, ((1,), (0,))) + qkv_bias).astype(BF16)
    queries = projected[:, :head_cols]
    key_rows = projected[:, head_cols : 2 * head_cols]
    value_rows = projected[:, 2 * head_cols :]
    mixed, log_totals = attention_forward(queries, key_rows, value_rows, length)
    attn_local = scatter_tensor(mixed, out_full, 2)
    first_out, first_normed, first_inverse = norm_rows(
        tokens.astype(F32) + (attn_local + out_bias), first_gain, first_shift
    )
    seq_first = gather_tensor(first_out.astype(BF16), 3)
    up_cols = lax.dynamic_slice_in_dim(up_bias, unit_start, unit_cols, 0)
    pre_act = mm(seq_first, up_full, ((1,), (0,))) + up_cols
    activated = gelu_tanh(pre_act).astype(BF16)
    ffn_local = scatter_tensor(activated, down_full, 4)
    second_in = first_out + (ffn_local + down_bias)
    layer_out, second_normed, second_inverse = norm_rows(second_in, second_gain, second_shift)
    upstream = cotangent.astype(F32) * row_valid[:, None].astype(F32)
    grad_second, gain_two_part, shift_two_part = norm_back(
        upstream, second_normed, second_inverse, second_gain
    )
    ffn_grad = grad_second.astype(BF16)
    down_bias_part = jnp.sum(ffn_grad.astype(F32), axis=0)
    unused_value, gelu_pull = jax.vjp(gelu_tanh, pre_act)
    seq_ffn_grad = gather_tensor(ffn_grad, 5)
    act_grad = mm(seq_ffn_grad, down_full, ((1,), (0,)))
    pre_grad = gelu_pull(act_grad)[0].astype(BF16)
    first_back = scatter_tensor(pre_grad, up_full, 6)
    up_bias_part = jnp.sum(pre_grad.astype(F32), axis=0)
    down_grad = mm(seq_ffn_grad, activated, ((0,), (0,))).astype(BF16)
    up_grad = mm(seq_first, pre_grad, ((0,), (0,))).astype(BF16)
    grad_first, gain_one_part, shift_one_part = norm_back(
        grad_second + first_back, first_normed, first_inverse, first_gain
    )
    attn_grad = grad_first.astype(BF16)
    out_bias_part = jnp.sum(attn_grad.astype(F32), axis=0)
    attn_grad, up_grad, down_grad = lax.optimization_barrier((attn_grad, up_grad, down_grad))
    grad_ud = lax.psum_scatter(
        jnp.concatenate([up_grad, down_grad], axis=1), "dp", scatter_dimension=0, tiled=True
    )
    seq_attn_grad = gather_tensor(attn_grad, 7)
    out_grad = mm(seq_attn_grad, mixed, ((0,), (0,))).astype(BF16)
    mixed_grad = mm(seq_attn_grad, out_full, ((1,), (0,))).astype(BF16)
    query_grad, key_grad, value_grad = attention_backward(
        queries, key_rows, value_rows, mixed_grad, log_totals, length
    )
    stacked = jnp.concatenate([query_grad, key_grad, value_grad], axis=1)
    qkv_grad = mm(seq_tokens, stacked, ((0,), (0,))).astype(BF16)
    zeros_heads = jnp.zeros((width,), F32)
    query_bias = lax.dynamic_update_slice(
        zeros_heads, jnp.sum(query_grad.astype(F32), axis=0), (head_start,)
    )
    value_bias = lax.dynamic_update_slice(
        zeros_heads, jnp.sum(value_grad.astype(F32), axis=0), (head_start,)
    )
    up_bias_full = lax.dynamic_update_slice(
        jnp.zeros((up_bias.shape[0],), F32), up_bias_part, (unit_start,)
    )
    small = jnp.concatenate(
        [
            item.reshape(ways, -1)
            for item in (
                query_bias,
                value_bias,
                out_bias_part,
                gain_one_part,
                shift_one_part,
                up_bias_full,
                down_bias_part,
                gain_two_part,
                shift_two_part,
            )
        ],
        axis=1,
    )
    bits_wide = small.shape[1]
    padded = -(-bits_wide // 1024) * 1024
    small = jnp.pad(small, ((0, 0), (0, padded - bits_wide))).reshape(ways, -1, 128)
    grads = jnp.concatenate([qkv_grad, out_grad], axis=1).reshape(-1, depth, 4 * head_cols)
    token_back, grad_qo, small = tail(stacked, qkv_full, grads, small)
    small = small.reshape(-1)
    grad_tokens = grad_first + token_back
    share = width // ways
    cuts = [0]
    for size in (share, share, share, share, share, up_bias.shape[0] // ways, share, share, share):
        cuts.append(cuts[-1] + size)
    bits = [small[cuts[i] : cuts[i + 1]] for i in range(9)]
    grad_ud = grad_ud.astype(F32)
    grad_qkv = jnp.stack([grad_qo[:, i * head_cols : (i + 1) * head_cols] for i in range(3)])
    return (
        layer_out.astype(BF16),
        grad_tokens,
        grad_qkv,
        jnp.stack([bits[0], bits[1]]),
        grad_qo[:, 3 * head_cols :].T,
        bits[2],
        bits[3],
        bits[4],
        grad_ud[:, :unit_cols],
        bits[5],
        grad_ud[:, unit_cols:].T,
        bits[6],
        bits[7],
        bits[8],
    )


def solution(mesh):
    both = ("dp", "tensor")
    return jax.shard_map(
        per_device,
        mesh=mesh,
        in_specs=(
            P(both, None),
            P("dp"),
            P(None, "dp", "tensor"),
            P(),
            P("tensor", "dp"),
            P(),
            P(),
            P(),
            P("dp", "tensor"),
            P(),
            P("tensor", "dp"),
            P(),
            P(),
            P(),
            P(both, None),
        ),
        out_specs=(
            P(both, None),
            P(both, None),
            P(None, "dp", "tensor"),
            P(None, both),
            P("tensor", "dp"),
            P(both),
            P(both),
            P(both),
            P("dp", "tensor"),
            P(both),
            P("tensor", "dp"),
            P(both),
            P(both),
            P(both),
        ),
        check_vma=False,
    )
```

```python
import math

import jax
import jax.numpy as jnp
from jax import lax
from jax.experimental import pallas as pl
from jax.experimental.pallas import tpu as pltpu
from jax.sharding import PartitionSpec as P

HEAD = 64
NEGATIVE = -1e30
EPSILON = 1e-05
F32 = jnp.float32
BF16 = jnp.bfloat16


def gelu_tanh(values):
    bracket = 0.7978845608028654 * (values + 0.044715 * values * values * values)
    return 0.5 * values * (1.0 + jnp.tanh(bracket))


def norm_rows(hidden, scaling, offset):
    centered = hidden - jnp.mean(hidden, axis=-1, keepdims=True)
    inverse = lax.rsqrt(jnp.mean(centered * centered, axis=-1, keepdims=True) + EPSILON)
    normed = centered * inverse
    return (normed * scaling + offset, normed, inverse)


def norm_back(upstream, normed, inverse, scaling):
    scaled = upstream * scaling
    bracket = (
        scaled
        - jnp.mean(scaled, axis=-1, keepdims=True)
        - normed * jnp.mean(scaled * normed, axis=-1, keepdims=True)
    )
    return (inverse * bracket, jnp.sum(upstream * normed, axis=0), jnp.sum(upstream, axis=0))


def mm(left, right, dims):
    return lax.dot_general(left, right, (dims, ((), ())), preferred_element_type=F32)


MESH = pl.DeviceIdType.MESH
PARTS = 4
STEPS = 4


def remote(src, dst, send, recv, where):
    return pltpu.make_async_remote_copy(
        src_ref=src, dst_ref=dst, send_sem=send, recv_sem=recv, device_id=where, device_id_type=MESH
    )


def neighbours():
    me = lax.axis_index("tensor")
    partner = me + 1 - 2 * (me % 2)
    return me, partner, (me + 2) % PARTS, (partner + 2) % PARTS


def greet(count, where):
    barrier = pltpu.get_barrier_semaphore()

    def one(k, carry):
        pl.semaphore_signal(barrier, inc=1, device_id=where(k), device_id_type=MESH)
        return carry

    lax.fori_loop(0, count, one, 0)
    pl.semaphore_wait(barrier, count)


def loop(count, body):
    def step(k, carry):
        body(k)
        return carry

    lax.fori_loop(0, count, step, 0)


class RowGather:
    semaphores = [pltpu.SemaphoreType.DMA((2, STEPS))] * 2 + [pltpu.SemaphoreType.DMA((2,))]

    def __init__(self, mine, seq, cross_sems, relay_sems, own_sems):
        self.mine, self.seq = mine, seq
        self.cross_sems, self.relay_sems, self.own_sems = cross_sems, relay_sems, own_sems
        self.me, self.partner, self.cross, self.diag = neighbours()
        self.rows = mine.shape[0] // STEPS

    def cut(self, k):
        return pl.ds(pl.multiple_of(k * self.rows, self.rows), self.rows)

    def crossing(self, k):
        return remote(
            self.mine.at[self.cut(k)],
            self.seq.at[self.me, self.cut(k)],
            self.cross_sems.at[0, k],
            self.cross_sems.at[1, k],
            {"tensor": self.cross},
        )

    def relay(self, k):
        block = self.seq.at[self.cross, self.cut(k)]
        return remote(
            block,
            block,
            self.relay_sems.at[0, k],
            self.relay_sems.at[1, k],
            {"tensor": self.partner},
        )

    def own(self):
        return remote(
            self.mine,
            self.seq.at[self.me],
            self.own_sems.at[0],
            self.own_sems.at[1],
            {"tensor": self.partner},
        )

    def start(self):
        loop(STEPS, lambda k: self.crossing(k).start())
        self.own().start()
        self.seq[self.me] = self.mine[...]

    def finish(self):
        def arrive(k):
            self.crossing(k).wait_recv()
            self.relay(k).start()

        loop(STEPS, arrive)
        self.own().wait()
        loop(STEPS, lambda k: self.crossing(k).wait_send())
        loop(STEPS, lambda k: self.relay(k).wait())


def greet_pair():
    me, partner, cross, diag = neighbours()
    greet(2, lambda k: {"tensor": partner + k * (cross - partner)})


def vmem():
    return pl.BlockSpec(memory_space=pltpu.VMEM)


def gather_kernel(mine, seq, cross_sems, relay_sems, own_sems):
    greet_pair()
    rows = RowGather(mine, seq, cross_sems, relay_sems, own_sems)
    rows.start()
    rows.finish()


def gather_tensor(rows, ident):
    count, width = rows.shape
    size = PARTS * count * width * 2
    seq = pl.pallas_call(
        gather_kernel,
        out_shape=jax.ShapeDtypeStruct((PARTS, count, width), rows.dtype),
        in_specs=[vmem()],
        out_specs=vmem(),
        scratch_shapes=RowGather.semaphores,
        cost_estimate=pl.CostEstimate(flops=0, bytes_accessed=20 * size, transcendentals=0),
        compiler_params=pltpu.CompilerParams(collective_id=ident, has_side_effects=True),
        name=f"gather_rows_{ident}",
    )(rows)
    return seq.reshape(PARTS * count, width)


def start_kernel(tokens, weight, seq, full, cross_sems, relay_sems, own_sems, weight_sems):
    place, count = lax.axis_index("dp"), lax.axis_size("dp")
    me, partner, cross, diag = neighbours()
    barrier = pltpu.get_barrier_semaphore()
    for where in (partner, cross):
        pl.semaphore_signal(barrier, inc=1, device_id={"tensor": where}, device_id_type=MESH)
    loop(
        count - 1,
        lambda k: pl.semaphore_signal(
            barrier, inc=1, device_id={"dp": (place + 1 + k) % count}, device_id_type=MESH
        ),
    )
    pl.semaphore_wait(barrier, count + 1)
    rows = RowGather(tokens, seq, cross_sems, relay_sems, own_sems)

    def piece(k):
        return remote(
            weight,
            full.at[place],
            weight_sems.at[0, k],
            weight_sems.at[1, k],
            {"dp": (place + 1 + k) % count},
        )

    loop(count - 1, lambda k: piece(k).start())
    rows.start()
    full[place] = weight[...]
    rows.finish()
    loop(count - 1, lambda k: piece(k).wait())


def start_gather(tokens, weight):
    count, width = tokens.shape
    ways = lax.axis_size("dp")
    seq, full = pl.pallas_call(
        start_kernel,
        out_shape=(
            jax.ShapeDtypeStruct((PARTS, count, width), tokens.dtype),
            jax.ShapeDtypeStruct((ways,) + weight.shape, weight.dtype),
        ),
        in_specs=[vmem()] * 2,
        out_specs=(vmem(), vmem()),
        scratch_shapes=RowGather.semaphores + [pltpu.SemaphoreType.DMA((2, ways - 1))],
        cost_estimate=pl.CostEstimate(flops=0, bytes_accessed=60 << 20, transcendentals=0),
        compiler_params=pltpu.CompilerParams(collective_id=1, has_side_effects=True),
        name="start_gather",
    )(tokens, weight)
    return seq.reshape(PARTS * count, width), full.reshape(-1, weight.shape[1])


class Scatter:
    def __init__(self, left, weight, out, pair_out, pair_in, over_out, over_in, pair_sems, over_sems):
        self.left, self.weight, self.out = left, weight, out
        self.pair_out, self.pair_in = pair_out, pair_in
        self.over_out, self.over_in = over_out, over_in
        self.pair_sems, self.over_sems = pair_sems, over_sems
        self.me, self.partner, self.cross, self.diag = neighbours()
        self.rows = left.shape[1] // STEPS

    @staticmethod
    def scratch(rows, width):
        return [
            pltpu.VMEM((2, rows, width), BF16),
            pltpu.VMEM((2, rows, width), BF16),
            pltpu.VMEM((rows, width), BF16),
            pltpu.VMEM((rows, width), BF16),
            pltpu.SemaphoreType.DMA((2, 2, STEPS)),
            pltpu.SemaphoreType.DMA((2, STEPS)),
        ]

    def cut(self, k):
        return pl.ds(pl.multiple_of(k * self.rows, self.rows), self.rows)

    def pair(self, which, k):
        return remote(
            self.pair_out.at[which, self.cut(k)],
            self.pair_in.at[which, self.cut(k)],
            self.pair_sems.at[0, which, k],
            self.pair_sems.at[1, which, k],
            {"tensor": self.partner},
        )

    def over(self, k):
        return remote(
            self.over_out.at[self.cut(k)],
            self.over_in.at[self.cut(k)],
            self.over_sems.at[0, k],
            self.over_sems.at[1, k],
            {"tensor": self.cross},
        )

    def product(self, block, k):
        return mm(self.left[block, self.cut(k)], self.weight[...], ((1,), (1,)))

    def run(self):
        def away(which, block):
            def body(k):
                self.pair_out[which, self.cut(k)] = self.product(block, k).astype(BF16)
                self.pair(which, k).start()

            return body

        def across(k):
            part = self.product(self.cross, k)
            self.pair(0, k).wait_recv()
            part = part + self.pair_in[0, self.cut(k)].astype(F32)
            self.over_out[self.cut(k)] = part.astype(BF16)
            self.over(k).start()

        def home(k):
            part = self.product(self.me, k)
            self.pair(1, k).wait_recv()
            self.out[self.cut(k)] = part + self.pair_in[1, self.cut(k)].astype(F32)

        def close(k):
            self.over(k).wait_recv()
            self.out[self.cut(k)] = self.out[self.cut(k)] + self.over_in[self.cut(k)].astype(F32)

        loop(STEPS, away(0, self.diag))
        loop(STEPS, across)
        loop(STEPS, away(1, self.partner))
        loop(STEPS, home)
        loop(STEPS, close)
        for which in range(2):
            loop(STEPS, lambda k: self.pair(which, k).wait_send())
        loop(STEPS, lambda k: self.over(k).wait_send())


def scatter_kernel(left, weight, out, *scratch):
    greet_pair()
    Scatter(left, weight, out, *scratch).run()


def scatter_tensor(left, weight, ident):
    rows, inner = left.shape[0] // PARTS, left.shape[1]
    width = weight.shape[0]
    return pl.pallas_call(
        scatter_kernel,
        out_shape=jax.ShapeDtypeStruct((rows, width), F32),
        in_specs=[vmem()] * 2,
        out_specs=vmem(),
        scratch_shapes=Scatter.scratch(rows, width),
        cost_estimate=pl.CostEstimate(
            flops=2 * PARTS * rows * inner * width, bytes_accessed=60 << 20, transcendentals=0
        ),
        compiler_params=pltpu.CompilerParams(collective_id=ident, has_side_effects=True),
        name=f"scatter_rows_{ident}",
    )(left.reshape(PARTS, rows, inner), weight)


def tail_kernel(left, weight, grads, small, out, grads_out, small_out, *scratch):
    scatter_scratch, (grads_in, small_in, grad_sems, small_sems) = scratch[:6], scratch[6:]
    place, count = lax.axis_index("dp"), lax.axis_size("dp")
    me = place * PARTS + lax.axis_index("tensor")
    ways = count * PARTS

    def rank(k):
        peer = (me + 1 + k) % ways
        return {"dp": peer // PARTS, "tensor": peer % PARTS}

    greet(ways - 1, rank)

    def grad(k):
        peer = (place + 1 + k) % count
        return remote(
            grads.at[peer], grads_in.at[k], grad_sems.at[0, k], grad_sems.at[1, k], {"dp": peer}
        )

    def bit(k):
        peer = (me + 1 + k) % ways
        return remote(
            small.at[peer], small_in.at[k], small_sems.at[0, k], small_sems.at[1, k], rank(k)
        )

    loop(count - 1, lambda k: grad(k).start())
    loop(ways - 1, lambda k: bit(k).start())
    Scatter(left, weight, out, *scatter_scratch).run()
    small_out[...] = small[me]

    def add_bit(k):
        bit(k).wait()
        small_out[...] = small_out[...] + small_in[k]

    loop(ways - 1, add_bit)
    grads_out[...] = grads[place].astype(F32)

    def add_grad(k):
        grad(k).wait()
        grads_out[...] = grads_out[...] + grads_in[k].astype(F32)

    loop(count - 1, add_grad)


def tail(left, weight, grads, small):
    rows, inner = left.shape[0] // PARTS, left.shape[1]
    width = weight.shape[0]
    count, ways = grads.shape[0], small.shape[0]
    return pl.pallas_call(
        tail_kernel,
        out_shape=(
            jax.ShapeDtypeStruct((rows, width), F32),
            jax.ShapeDtypeStruct(grads.shape[1:], F32),
            jax.ShapeDtypeStruct(small.shape[1:], F32),
        ),
        in_specs=[vmem()] * 4,
        out_specs=(vmem(),) * 3,
        scratch_shapes=Scatter.scratch(rows, width)
        + [
            pltpu.VMEM((count - 1,) + grads.shape[1:], BF16),
            pltpu.VMEM((ways - 1,) + small.shape[1:], F32),
            pltpu.SemaphoreType.DMA((2, count - 1)),
            pltpu.SemaphoreType.DMA((2, ways - 1)),
        ],
        cost_estimate=pl.CostEstimate(
            flops=2 * PARTS * rows * inner * width, bytes_accessed=90 << 20, transcendentals=0
        ),
        compiler_params=pltpu.CompilerParams(collective_id=9, has_side_effects=True),
        name="tail",
    )(left.reshape(PARTS, rows, inner), weight, grads, small)


CHUNK = 512
SLOPE = math.log2(math.e) / math.sqrt(HEAD)
SCALE = 1.0 / math.sqrt(HEAD)


def lanes(rows):
    return lax.broadcasted_iota(jnp.int32, (rows, 128), 1)


def window(ref, slot, rows):
    cols = ref[rows, pl.ds(slot // 2 * 128, 128)].astype(F32)
    return cols if slot % 2 == 0 else pltpu.roll(cols, HEAD, 1)


def pair_up(low, high):
    return jnp.where(lanes(low.shape[0]) < HEAD, low, pltpu.roll(high, HEAD, 1))


def chunk_at(k):
    return pl.ds(pl.multiple_of(k * CHUNK, CHUNK), CHUNK)


def head_at(h):
    return pl.ds(pl.multiple_of(h * HEAD, HEAD), HEAD)


def prepare_keys(length, packed, heads, queries, keys, rows):
    lane = lanes(CHUNK)
    start = rows * CHUNK + lax.broadcasted_iota(jnp.int32, (CHUNK, 128), 0)
    bias = jnp.where(start < length, 0.0, NEGATIVE)
    at = chunk_at(rows)
    for h in range(heads):
        query = window(packed, h, at)
        queries[h, at] = jnp.where(lane < HEAD, query, jnp.where(lane == HEAD, 1.0, 0.0)).astype(BF16)
        key = window(packed, heads + h, at)
        keys[h, at] = jnp.where(lane < HEAD, key, jnp.where(lane == HEAD, bias, 0.0)).astype(BF16)


def forward_kernel(heads, length, packed, mixed, logs, queries, keys, values_t, mixed_t):
    chunks = packed.shape[0] // CHUNK

    def prepare(k):
        prepare_keys(length[0], packed, heads, queries, keys, k)
        for h in range(heads):
            value = window(packed, 2 * heads + h, chunk_at(k))
            values_t[pl.ds(h * HEAD, HEAD), chunk_at(k)] = jnp.transpose(value)[:HEAD].astype(BF16)

    loop(chunks, prepare)

    def attend(step):
        h, block = step // chunks, step % chunks
        query = queries[h, chunk_at(block)]
        top = jnp.full((1, CHUNK), -jnp.inf, F32)
        total = jnp.zeros((1, CHUNK), F32)
        mix = jnp.zeros((HEAD, CHUNK), F32)
        for k in range(chunks):
            scores = mm(keys[h, pl.ds(k * CHUNK, CHUNK)], query, ((1,), (1,)))
            fresh = jnp.maximum(top, jnp.max(scores, axis=0, keepdims=True))
            expo = jnp.exp2(scores * SLOPE - fresh * SLOPE)
            keep = jnp.exp2((top - fresh) * SLOPE)
            total = total * keep + jnp.sum(expo, axis=0, keepdims=True)
            value = values_t[head_at(h), pl.ds(k * CHUNK, CHUNK)]
            mix = mix * keep + mm(value, expo.astype(BF16), ((1,), (0,)))
            top = fresh
        mixed_t[head_at(h), chunk_at(block)] = mix / total
        logs[h, :, chunk_at(block)] = jnp.broadcast_to(top * SLOPE + jnp.log2(total), (8, CHUNK))

    loop(heads * chunks, attend)
    spare = mixed_t.shape[0] - heads * HEAD
    if spare:
        mixed_t[pl.ds(heads * HEAD, spare)] = jnp.zeros((spare, mixed_t.shape[1]), F32)

    def collect(k):
        for pair in range(mixed_t.shape[0] // 128):
            part = mixed_t[pl.ds(pair * 128, 128), chunk_at(k)]
            mixed[chunk_at(k), pl.ds(pair * 128, 128)] = jnp.transpose(part).astype(BF16)

    loop(chunks, collect)


def attention_forward(packed, length, heads):
    rows = packed.shape[0]
    wide = -(-heads // 2) * 128
    pieces = heads * rows * rows
    return pl.pallas_call(
        lambda *refs: forward_kernel(heads, *refs),
        out_shape=(
            jax.ShapeDtypeStruct((rows, wide), BF16),
            jax.ShapeDtypeStruct((heads, 8, rows), F32),
        ),
        in_specs=[pl.BlockSpec(memory_space=pltpu.SMEM), vmem()],
        out_specs=(vmem(), vmem()),
        scratch_shapes=[
            pltpu.VMEM((heads, rows, 128), BF16),
            pltpu.VMEM((heads, rows, 128), BF16),
            pltpu.VMEM((wide, rows), BF16),
            pltpu.VMEM((wide, rows), F32),
        ],
        cost_estimate=pl.CostEstimate(
            flops=4 * pieces * 256, bytes_accessed=80 << 20, transcendentals=pieces
        ),
        name="attention_forward",
    )(length, packed)


def backward_kernel(
    heads, length, packed, mixed, grad, logs, out, sums, queries, keys, values, grads, keys_t, query_t,
    key_acc, value_acc,
):
    chunks = packed.shape[0] // CHUNK
    lane = lanes(CHUNK)

    def prepare(k):
        at = chunk_at(k)
        prepare_keys(length[0], packed, heads, queries, keys, k)
        for h in range(heads):
            key = window(packed, heads + h, at)
            keys_t[pl.ds(h * HEAD, HEAD), at] = jnp.transpose(key)[:HEAD].astype(BF16)
            value = window(packed, 2 * heads + h, at)
            ones = jnp.where(lane < HEAD + 3, 1.0, 0.0)
            values[h, at] = jnp.where(lane < HEAD, value, ones).astype(BF16)
            above = window(grad, h, at)
            product = jnp.where(lane < HEAD, above * window(mixed, h, at), 0.0)
            centre = jnp.sum(product, axis=1, keepdims=True)
            first = centre.astype(BF16).astype(F32)
            second = (centre - first).astype(BF16).astype(F32)
            third = centre - first - second
            extra = jnp.where(
                lane == HEAD, first, jnp.where(lane == HEAD + 1, second, jnp.where(lane == HEAD + 2, third, 0.0))
            )
            grads[h, at] = jnp.where(lane < HEAD, above, -extra).astype(BF16)
            key_acc[h, at] = jnp.zeros((CHUNK, 128), F32)
            value_acc[h, at] = jnp.zeros((CHUNK, 128), F32)

    loop(chunks, prepare)

    def attend(step):
        h, block = step // chunks, step % chunks
        query = queries[h, chunk_at(block)]
        above = grads[h, chunk_at(block)]
        log = logs[h, pl.ds(0, 1), chunk_at(block)]
        query_grad = jnp.zeros((HEAD, CHUNK), F32)
        for k in range(chunks):
            at = pl.ds(k * CHUNK, CHUNK)
            scores = mm(keys[h, at], query, ((1,), (1,)))
            probs = jnp.exp2(scores * SLOPE - log)
            centred = mm(values[h, at], above, ((1,), (1,)))
            score_grad = (probs * centred).astype(BF16)
            value_acc[h, at] += mm(probs.astype(BF16), above, ((1,), (0,)))
            key_acc[h, at] += mm(score_grad, query, ((1,), (0,)))
            query_grad = query_grad + mm(keys_t[head_at(h), at], score_grad, ((1,), (0,)))
        query_t[head_at(h), chunk_at(block)] = query_grad * SCALE

    loop(heads * chunks, attend)
    sums[...] = jnp.zeros_like(sums)
    spare = query_t.shape[0] - heads * HEAD
    if spare:
        query_t[pl.ds(heads * HEAD, spare)] = jnp.zeros((spare, query_t.shape[1]), F32)

    def collect(k):
        at = chunk_at(k)

        def slot(index):
            h = index % heads
            if index < heads:
                rows = jnp.transpose(query_t[pl.ds(h // 2 * 128, 128), at])
                return rows if h % 2 == 0 else pltpu.roll(rows, HEAD, 1)
            if index < 2 * heads:
                return key_acc[h, at] * SCALE
            if index < 3 * heads:
                return value_acc[h, at]
            return jnp.zeros((CHUNK, 128), F32)

        for pair in range(out.shape[1] // 128):
            part = pair_up(slot(2 * pair), slot(2 * pair + 1)).astype(BF16)
            out[at, pl.ds(pair * 128, 128)] = part
            sums[:, pl.ds(pair * 128, 128)] += jnp.sum(part.astype(F32), axis=0, keepdims=True)

    loop(chunks, collect)


def attention_backward(packed, mixed, grad, logs, length, heads):
    rows, width = packed.shape
    wide = -(-heads // 2) * 128
    pieces = heads * rows * rows
    return pl.pallas_call(
        lambda *refs: backward_kernel(heads, *refs),
        out_shape=(
            jax.ShapeDtypeStruct((rows, width), BF16),
            jax.ShapeDtypeStruct((8, width), F32),
        ),
        in_specs=[pl.BlockSpec(memory_space=pltpu.SMEM)] + [vmem()] * 4,
        out_specs=(vmem(), vmem()),
        scratch_shapes=[pltpu.VMEM((heads, rows, 128), BF16)] * 4
        + [pltpu.VMEM((wide, rows), BF16), pltpu.VMEM((wide, rows), F32)]
        + [pltpu.VMEM((heads, rows, 128), F32)] * 2,
        cost_estimate=pl.CostEstimate(
            flops=10 * pieces * 256, bytes_accessed=200 << 20, transcendentals=pieces
        ),
        name="attention_backward",
    )(length, packed, mixed, grad, logs)


def per_device(
    tokens,
    lengths,
    qkv_weight,
    qv_bias,
    out_weight,
    out_bias,
    first_gain,
    first_shift,
    up_weight,
    up_bias,
    down_weight,
    down_bias,
    second_gain,
    second_shift,
    cotangent,
):
    local_rows, width = tokens.shape
    piece = lax.axis_index("tensor")
    ways = lax.axis_size("dp") * lax.axis_size("tensor")
    head_cols = qkv_weight.shape[2]
    unit_cols = up_weight.shape[1]
    depth = up_weight.shape[0]
    length = lengths[0]
    heads = head_cols // HEAD
    pad_qkv = -(-3 * heads // 2) * 128 - 3 * head_cols
    pad_out = -(-heads // 2) * 128 - head_cols
    qkv_rows = jnp.pad(
        jnp.concatenate([qkv_weight[0], qkv_weight[1], qkv_weight[2]], axis=1), ((0, 0), (0, pad_qkv))
    )
    seq_tokens, qkv_full = start_gather(tokens, qkv_rows)
    out_rows = jnp.pad(out_weight.T, ((0, 0), (0, pad_out)))
    rest_rows = jnp.concatenate([up_weight, down_weight.T, out_rows], axis=1)
    rest_full = lax.all_gather(rest_rows, "dp", axis=0, tiled=True)
    up_full = rest_full[:, :unit_cols]
    down_full = rest_full[:, unit_cols : 2 * unit_cols]
    out_full = rest_full[:, 2 * unit_cols :]
    row_start = piece * local_rows
    row_valid = row_start + jnp.arange(local_rows, dtype=jnp.int32) < length
    head_start = piece * head_cols
    unit_start = piece * unit_cols
    bias_cols = lax.dynamic_slice_in_dim(qv_bias, head_start, head_cols, 1)
    qkv_bias = jnp.concatenate(
        [bias_cols[0], jnp.zeros((head_cols,), F32), bias_cols[1], jnp.zeros((pad_qkv,), F32)]
    )
    projected = (mm(seq_tokens, qkv_full, ((1,), (0,))) + qkv_bias).astype(BF16)
    mixed, logs = attention_forward(projected, lengths, heads)
    attn_local = scatter_tensor(mixed, out_full, 2)
    first_out, first_normed, first_inverse = norm_rows(
        tokens.astype(F32) + (attn_local + out_bias), first_gain, first_shift
    )
    seq_first = gather_tensor(first_out.astype(BF16), 3)
    up_cols = lax.dynamic_slice_in_dim(up_bias, unit_start, unit_cols, 0)
    pre_act = mm(seq_first, up_full, ((1,), (0,))) + up_cols
    activated = gelu_tanh(pre_act).astype(BF16)
    ffn_local = scatter_tensor(activated, down_full, 4)
    second_in = first_out + (ffn_local + down_bias)
    layer_out, second_normed, second_inverse = norm_rows(second_in, second_gain, second_shift)
    upstream = cotangent.astype(F32) * row_valid[:, None].astype(F32)
    grad_second, gain_two_part, shift_two_part = norm_back(
        upstream, second_normed, second_inverse, second_gain
    )
    ffn_grad = grad_second.astype(BF16)
    down_bias_part = jnp.sum(ffn_grad.astype(F32), axis=0)
    unused_value, gelu_pull = jax.vjp(gelu_tanh, pre_act)
    seq_ffn_grad = gather_tensor(ffn_grad, 5)
    act_grad = mm(seq_ffn_grad, down_full, ((1,), (0,)))
    pre_grad = gelu_pull(act_grad)[0].astype(BF16)
    first_back = scatter_tensor(pre_grad, up_full, 6)
    up_bias_part = jnp.sum(pre_grad.astype(F32), axis=0)
    down_grad = mm(seq_ffn_grad, activated, ((0,), (0,))).astype(BF16)
    up_grad = mm(seq_first, pre_grad, ((0,), (0,))).astype(BF16)
    grad_first, gain_one_part, shift_one_part = norm_back(
        grad_second + first_back, first_normed, first_inverse, first_gain
    )
    attn_grad = grad_first.astype(BF16)
    out_bias_part = jnp.sum(attn_grad.astype(F32), axis=0)
    attn_grad, up_grad, down_grad = lax.optimization_barrier((attn_grad, up_grad, down_grad))
    grad_ud = lax.psum_scatter(
        jnp.concatenate([up_grad, down_grad], axis=1), "dp", scatter_dimension=0, tiled=True
    )
    seq_attn_grad = gather_tensor(attn_grad, 7)
    out_grad = mm(seq_attn_grad, mixed, ((0,), (0,))).astype(BF16)
    mixed_grad = mm(seq_attn_grad, out_full, ((1,), (0,))).astype(BF16)
    stacked, sums = attention_backward(projected, mixed, mixed_grad, logs, lengths, heads)
    qkv_grad = mm(seq_tokens, stacked, ((0,), (0,))).astype(BF16)
    zeros_heads = jnp.zeros((width,), F32)
    query_bias = lax.dynamic_update_slice(
        zeros_heads, sums[0, :head_cols], (head_start,)
    )
    value_bias = lax.dynamic_update_slice(
        zeros_heads, sums[0, 2 * head_cols : 3 * head_cols], (head_start,)
    )
    up_bias_full = lax.dynamic_update_slice(
        jnp.zeros((up_bias.shape[0],), F32), up_bias_part, (unit_start,)
    )
    small = jnp.concatenate(
        [
            item.reshape(ways, -1)
            for item in (
                query_bias,
                value_bias,
                out_bias_part,
                gain_one_part,
                shift_one_part,
                up_bias_full,
                down_bias_part,
                gain_two_part,
                shift_two_part,
            )
        ],
        axis=1,
    )
    bits_wide = small.shape[1]
    padded = -(-bits_wide // 1024) * 1024
    small = jnp.pad(small, ((0, 0), (0, padded - bits_wide))).reshape(ways, -1, 128)
    grads = jnp.concatenate([qkv_grad, out_grad], axis=1)
    grads = grads.reshape(-1, depth, grads.shape[1])
    token_back, grad_qo, small = tail(stacked, qkv_full, grads, small)
    small = small.reshape(-1)
    grad_tokens = grad_first + token_back
    share = width // ways
    cuts = [0]
    for size in (share, share, share, share, share, up_bias.shape[0] // ways, share, share, share):
        cuts.append(cuts[-1] + size)
    bits = [small[cuts[i] : cuts[i + 1]] for i in range(9)]
    grad_ud = grad_ud.astype(F32)
    grad_qkv = jnp.stack([grad_qo[:, i * head_cols : (i + 1) * head_cols] for i in range(3)])
    return (
        layer_out.astype(BF16),
        grad_tokens,
        grad_qkv,
        jnp.stack([bits[0], bits[1]]),
        grad_qo[:, 3 * head_cols + pad_qkv :][:, :head_cols].T,
        bits[2],
        bits[3],
        bits[4],
        grad_ud[:, :unit_cols],
        bits[5],
        grad_ud[:, unit_cols:].T,
        bits[6],
        bits[7],
        bits[8],
    )


def solution(mesh):
    both = ("dp", "tensor")
    return jax.shard_map(
        per_device,
        mesh=mesh,
        in_specs=(
            P(both, None),
            P("dp"),
            P(None, "dp", "tensor"),
            P(),
            P("tensor", "dp"),
            P(),
            P(),
            P(),
            P("dp", "tensor"),
            P(),
            P("tensor", "dp"),
            P(),
            P(),
            P(),
            P(both, None),
        ),
        out_specs=(
            P(both, None),
            P(both, None),
            P(None, "dp", "tensor"),
            P(None, both),
            P("tensor", "dp"),
            P(both),
            P(both),
            P(both),
            P("dp", "tensor"),
            P(both),
            P("tensor", "dp"),
            P(both),
            P(both),
            P(both),
        ),
        check_vma=False,
    )
```
